128 devices in a mesh: groups: 4 (over x, y), freq: 16 (over z), mgrp: 2 (over core).
Axes of the slice: x: 2, y: 2, z: 16, core: 2. Of those that a mesh axis runs over, the one named last changes fastest.
The devices are a block of a 8x8x16 slice.
Arguments:
- seeds: int32 [128, 1024], P('groups', 'mgrp'), parts along dimension 0, may hold values from 0 to 1073741823
- noise_amp: float32 [1024, 512], P(('groups', 'freq')), parts along dimension 0, may hold values from 0.3 to 3
- singular_projection: bfloat16 [128, 256, 16, 512], P('groups', 'freq'), parts along dimension 0, may hold values from -0.25 to 0.25
- kl_vecs: bfloat16 [128, 1536, 4096], P(('groups', 'freq'), 'mgrp'), parts along dimension 0, may hold values from -0.09375 to 0.09375
- m_order: int32 [128], P('groups'), parts along dimension 0, may hold values from 0 to 31, each once
- mode_counts: int32 [128], P('groups'), parts along dimension 0, may hold values from 384 to 1536, as said below
Outputs:
- kl_coeffs: bfloat16 [128, 1536, 1024], P(('groups', 'freq'), None, 'mgrp'), parts along dimension 0
The draws below stay inside these ranges and needn't reach their ends.
There are 4 independent parts, one for each index of `groups`. The reference program is written for one: setup_inputs(seed, part) draws one part's arguments, and reference() takes and returns one part's arrays. A program takes and returns all parts, laid end to end along the dimension named above; each array names one. Nothing has to cross between parts.
Inputs may be any that keep to these rules, and one draw needn't show every extreme that they name: `m_order`: each m appears in exactly one slot. `mode_counts`: some m keeps all 1536 modes.
All inputs are finite; a program needn't handle non-finite values.
Results may differ from the reference program's by a relative error of at most 0.0058.
Values may be sent and summed in bfloat16 or wider, within the bound.
No kernel may reach another device: no remote copies, remote signals or barrier semaphores. Data moves between devices by JAX's collectives and lax.ppermute only.
A program may use at most 192 MiB of HBM per device.

```python
import math
import jax
import jax.numpy as jnp
from jax import lax

NF = 256
SVD_MODES = 16
NB = 512
KL_MAX = 1536
REALS = 1024
SVD_LEN = 4096
MS = 32


def draw_mode_counts(key, part):
    counts = jax.random.randint(key, (MS,), KL_MAX // 4, KL_MAX + 1, dtype=jnp.int32)
    chosen = jax.random.randint(jax.random.fold_in(key, 7), (), 0, MS, dtype=jnp.int32)
    return jnp.where(jnp.arange(MS, dtype=jnp.int32) == chosen, KL_MAX, counts).astype(jnp.int32)


def set_ends(array, key, least, top_value):
    place = [jax.random.randint(jax.random.fold_in(key, axis), (), 0, length) for axis, length in enumerate(array.shape)]
    main_axis = array.shape.index(max(array.shape))
    beside = place[:main_axis] + [(place[main_axis] + 1) % array.shape[main_axis]] + place[main_axis + 1:]
    return array.at[tuple(place)].set(least).at[tuple(beside)].set(top_value)


def shard_levels(rng, shape, shards, least, top_value):
    def one(axis_at, shards_of):
        draws = jax.random.uniform(jax.random.fold_in(jax.random.fold_in(rng, 6), axis_at), (shards_of,), jnp.float32, least / len(shards), top_value / len(shards))
        return jnp.repeat(jnp.exp(draws), shape[axis_at] // shards_of).reshape((-1,) + (1,) * (len(shape) - axis_at - 1))

    level = one(*shards[0])
    for cut in shards[1:]:
        level = level * one(*cut)
    return level


def normal_values(key, dims, scale, reach, shards=(), held_as=jnp.bfloat16):
    loudness = shard_levels(key, dims, shards, -0.22, 0.18) if shards else 1.0
    result = jax.random.normal(key, dims, jnp.float32) * scale * loudness
    return jnp.minimum(jnp.maximum(result, -reach), reach).astype(held_as)


def setup_inputs(seed: int = 0, part: int = 0) -> dict:
    key_list = jax.random.split(jax.random.key(seed), 7)
    own_keys = jax.random.split(jax.random.fold_in(key_list[6], part), 7)
    seeds = set_ends(jax.random.randint(own_keys[0], (MS, REALS), 0, 1073741824), jax.random.fold_in(own_keys[0], 1), 0, 1073741823).astype(jnp.int32)
    noise_amp = jnp.clip(jnp.exp(math.log(3.0) - 2.3025851 * jax.random.uniform(own_keys[1], (NF, NB), jnp.float32) ** shard_levels(own_keys[1], (NF, NB), ((0, 16),), -0.2, 0.2)), 0.3, 3.0)
    singular_projection = normal_values(own_keys[2], (MS, NF, SVD_MODES, NB), NB ** -0.5, 0.25, ((1, 16),))
    kl_vecs = normal_values(own_keys[3], (MS, KL_MAX, SVD_LEN), SVD_LEN ** -0.5, 0.09375, ((0, 16), (1, 2)))
    m_order = jax.random.permutation(own_keys[4], MS).astype(jnp.int32)
    mode_counts = draw_mode_counts(jax.random.fold_in(jax.random.fold_in(key_list[6], part), 71), part)
    return {"seeds": seeds, "noise_amp": noise_amp, "singular_projection": singular_projection, "kl_vecs": kl_vecs, "m_order": m_order, "mode_counts": mode_counts}


golden = 1640531527


def scramble(hashed_seed):
    hashed_seed = hashed_seed ^ ((hashed_seed >> 16) & 65535)
    hashed_seed = hashed_seed * 2146121005
    hashed_seed = hashed_seed ^ ((hashed_seed >> 15) & 131071)
    hashed_seed = hashed_seed * 1863026059
    hashed_seed = hashed_seed ^ ((hashed_seed >> 16) & 65535)
    return ((hashed_seed & 65535).astype(jnp.float32) - 32767.5) / 18918.0


def reference(seeds, noise_amp, singular_projection, kl_vecs, m_order, mode_counts):
    channel_index = jnp.arange(NF * NB, dtype=jnp.int32).reshape(NF, NB)
    mode_row_block = jnp.arange(KL_MAX, dtype=jnp.int32)

    def project(m_number):
        noise_draw = scramble(seeds[m_number][None, None, :] + channel_index[:, :, None] * golden)
        visible = (noise_amp[:, :, None] * noise_draw).astype(jnp.bfloat16)
        stacked = jnp.einsum("fkb,fbr->fkr", singular_projection[m_number].astype(jnp.float32), visible.astype(jnp.float32), precision=lax.Precision.HIGHEST)
        return stacked.astype(jnp.bfloat16).reshape(NF * SVD_MODES, REALS)

    def one_slot(position_index):
        m_number = m_order[position_index]
        vectors = project(m_number)
        coeffs = jnp.dot(kl_vecs[position_index], vectors, preferred_element_type=jnp.float32)
        kept_rows = mode_row_block[:, None] < mode_counts[m_number]
        return jnp.where(kept_rows, coeffs, jnp.float32(0.0)).astype(jnp.bfloat16)

    return lax.map(one_slot, jnp.arange(MS, dtype=jnp.int32))
```

```python
import functools

import jax
import jax.numpy as jnp
from jax import lax
from jax.experimental import pallas as pl
from jax.experimental.pallas import tpu as pltpu
from jax.sharding import PartitionSpec as P

golden = 1640531527


def wrap(value):
    value &= 0xFFFFFFFF
    return value - (1 << 32) if value >= 1 << 31 else value


def draw_bits(x):
    x = x ^ lax.shift_right_logical(x, 16)
    x = x * 2146121005
    x = x ^ lax.shift_right_logical(x, 15)
    x = x * 1863026059
    x = x ^ lax.shift_right_logical(x, 16)
    return (x & 65535).astype(jnp.float32)


def weigh_body(m_ref, w_ref, amp_ref, *outs):
    for place, out in enumerate(outs):

        @pl.when(pl.program_id(0) == place)
        def _():
            for chan in range(w_ref.shape[1]):
                scale = amp_ref[chan : chan + 1, :] * (1.0 / 18918.0)
                out[chan] = (w_ref[0, chan].astype(jnp.float32) * scale).astype(jnp.bfloat16)


def weigh(m_list, singular_projection, noise_amp):
    count = m_list.shape[0]
    chan, modes, pairs = singular_projection.shape[1:]
    return pl.pallas_call(
        weigh_body,
        out_shape=[jax.ShapeDtypeStruct((chan, modes, pairs), jnp.bfloat16)] * count,
        grid_spec=pltpu.PrefetchScalarGridSpec(
            num_scalar_prefetch=1,
            grid=(count,),
            in_specs=[
                pl.BlockSpec((1, chan, modes, pairs), lambda i, m: (m[i], 0, 0, 0)),
                pl.BlockSpec((chan, pairs), lambda i, m: (0, 0)),
            ],
            out_specs=[pl.BlockSpec((chan, modes, pairs), lambda i, m: (0, 0, 0))] * count,
        ),
        compiler_params=pltpu.CompilerParams(dimension_semantics=("arbitrary",)),
        name="weigh",
    )(m_list, singular_projection, noise_amp)


def project_body(chan_ref, seed_ref, *refs, parts, reals):
    w_refs, out_ref = refs[:parts], refs[-1]
    step = pl.program_id(0)
    chan_each = pl.num_programs(0) // parts
    w = w_refs[0][0]
    for place in range(1, parts):
        w = jnp.where(step >= place * chan_each, w_refs[place][0], w)
    pairs = w.shape[1]
    centre = 32767.5 * jnp.sum(w.astype(jnp.float32), axis=1, keepdims=True)
    tile = 256
    base = (lax.broadcasted_iota(jnp.int32, (8, tile), 0) + chan_ref[step] * pairs) * golden
    for r0 in range(0, reals, tile):
        start = seed_ref[:, r0 : r0 + tile] + base
        total = None
        for b0 in range(0, pairs, tile):
            bits = jnp.concatenate([draw_bits(start + wrap(b * golden)) for b in range(b0, b0 + tile, 8)], 0)
            piece = jnp.dot(w[:, b0 : b0 + tile], bits.astype(jnp.bfloat16), preferred_element_type=jnp.float32)
            total = piece if total is None else total + piece
        out_ref[0, :, r0 : r0 + tile] = (total - centre).astype(jnp.bfloat16)


def project(chan_list, seed_row, weights, vectors):
    parts = len(weights)
    chan, modes, pairs = weights[0].shape
    reals = seed_row.shape[1]

    def weight_spec(place):
        return pl.BlockSpec((1, modes, pairs), lambda i, c: (jnp.clip(i - place * chan, 0, chan - 1), 0, 0))

    in_specs = [pl.BlockSpec((8, reals), lambda i, c: (0, 0))]
    in_specs += [weight_spec(place) for place in range(parts)]
    operands = [chan_list, seed_row, *weights]
    aliases = {}
    if not isinstance(vectors, tuple):
        in_specs.append(pl.BlockSpec(memory_space=pl.ANY))
        aliases = {len(operands): 0}
        operands.append(vectors)
        shape = vectors.shape
    else:
        shape = vectors
    return pl.pallas_call(
        functools.partial(project_body, parts=parts, reals=reals),
        out_shape=jax.ShapeDtypeStruct(shape, jnp.bfloat16),
        grid_spec=pltpu.PrefetchScalarGridSpec(
            num_scalar_prefetch=1,
            grid=(parts * chan,),
            in_specs=in_specs,
            out_specs=pl.BlockSpec((1, modes, reals), lambda i, c: (c[i], 0, 0)),
        ),
        input_output_aliases=aliases,
        compiler_params=pltpu.CompilerParams(dimension_semantics=("arbitrary",)),
        name="project",
    )(*operands)


def transform_body(info_ref, near_ref, far_ref, vec_ref, out_ref, *, rows, blocks):
    step = pl.program_id(0)
    first = step * rows
    limit = info_ref[1]
    mine = step // blocks == info_ref[0]

    def run(kl_ref):
        coeffs = jnp.dot(kl_ref[0], vec_ref[...], preferred_element_type=jnp.float32)
        row = first + lax.broadcasted_iota(jnp.int32, coeffs.shape, 0)
        out_ref[0] = jnp.where(row < limit, coeffs, 0.0).astype(jnp.bfloat16)

    @pl.when((first < limit) & mine)
    def _():
        run(near_ref)

    @pl.when((first < limit) & jnp.logical_not(mine))
    def _():
        run(far_ref)

    @pl.when(first >= limit)
    def _():
        out_ref[...] = jnp.zeros(out_ref.shape, out_ref.dtype)


def transform(info, kl_near, kl_far, vectors, half, halves, slots):
    held, length = kl_near.shape[1:]
    reals = vectors.shape[1] // halves
    rows = 256
    blocks = held // rows

    def near(i, s):
        return (s[0], jnp.clip(i - s[0] * blocks, 0, blocks - 1), 0)

    def far(i, s):
        return (s[0], jnp.clip(i - (1 - s[0]) * blocks, 0, blocks - 1), 0)

    return pl.pallas_call(
        functools.partial(transform_body, rows=rows, blocks=blocks),
        out_shape=jax.ShapeDtypeStruct((slots, 2 * held, reals), jnp.bfloat16),
        grid_spec=pltpu.PrefetchScalarGridSpec(
            num_scalar_prefetch=1,
            grid=(2 * blocks,),
            in_specs=[
                pl.BlockSpec((1, rows, length), near),
                pl.BlockSpec((1, rows, length), far),
                pl.BlockSpec((length, reals), lambda i, s: (0, half)),
            ],
            out_specs=pl.BlockSpec((1, rows, reals), lambda i, s: (s[0] * (slots - 1), i, 0)),
        ),
        compiler_params=pltpu.CompilerParams(dimension_semantics=("arbitrary",), vmem_limit_bytes=48 * 2**20),
        name="transform",
    )(info, kl_near, kl_far, vectors)


def per_device(seeds, noise_amp, singular_projection, kl_vecs, m_order, mode_counts):
    freq_count = lax.axis_size("freq")
    d = lax.axis_index("freq")
    core = lax.axis_index("mgrp")
    chan, modes, pairs = singular_projection.shape[1:]
    order_grid = m_order.reshape(freq_count, 2)
    swap = [(0, 1), (1, 0)]

    half_way = freq_count // 2
    groups = [[0]] + [[k, -k] for k in range(1, half_way)] + [[half_way]]
    shifts = [s for g in groups for s in g]
    dest_m = [order_grid[(d + s) % freq_count, core] for s in shifts]
    first = weigh(jnp.stack(dest_m[:3]), singular_projection, noise_amp)
    rest = weigh(jnp.stack(dest_m[3:]), singular_projection, noise_amp)
    weighed = dict(zip(shifts, [*first, *rest]))
    arrived = {0: weighed[0]}
    for s in shifts[1:]:
        arrived[s] = lax.ppermute(weighed[s], "freq", [(i, (i + s) % freq_count) for i in range(freq_count)])
    kl_far = lax.ppermute(kl_vecs, "mgrp", swap)

    own_m = order_grid[d, core]
    own_seeds = lax.dynamic_index_in_dim(seeds, own_m, 0)
    far_seeds = lax.ppermute(lax.dynamic_index_in_dim(seeds, order_grid[d, 1 - core], 0), "mgrp", swap)
    seed_row = jnp.broadcast_to(jnp.concatenate([own_seeds, far_seeds], 1), (8, 2 * own_seeds.shape[1]))

    vectors = (freq_count * chan, modes, seed_row.shape[1])
    for g in groups:
        chans = jnp.concatenate([(d - s) % freq_count * chan + jnp.arange(chan, dtype=jnp.int32) for s in g])
        vectors = project(chans, seed_row, [arrived[s] for s in g], vectors)

    limit = lax.dynamic_index_in_dim(mode_counts, own_m, 0, keepdims=False)
    info = jnp.stack([core, limit]).astype(jnp.int32)
    stacked = vectors.reshape(freq_count * chan * modes, -1)
    sent = transform(info, kl_vecs, kl_far, stacked, 1, 2, 1)
    got = lax.ppermute(sent, "mgrp", swap)
    kept = transform(info, kl_vecs, kl_far, stacked, 0, 2, 2)
    return lax.dynamic_update_slice_in_dim(kept, got, 1 - core, 0)


def solution(mesh):
    placed = (
        P("groups", "mgrp"),
        P(("groups", "freq"), None),
        P("groups", "freq", None, None),
        P(("groups", "freq"), "mgrp", None),
        P("groups"),
        P("groups"),
    )
    return jax.shard_map(
        per_device,
        mesh=mesh,
        in_specs=placed,
        out_specs=P(("groups", "freq"), None, "mgrp"),
        check_vma=False,
    )
```

```python
import functools

import jax
import jax.numpy as jnp
from jax import lax
from jax.experimental import pallas as pl
from jax.experimental.pallas import tpu as pltpu
from jax.sharding import PartitionSpec as P

golden = 1640531527


def wrap(value):
    value &= 0xFFFFFFFF
    return value - (1 << 32) if value >= 1 << 31 else value


def draw_bits(x):
    x = x ^ lax.shift_right_logical(x, 16)
    x = x * 2146121005
    x = x ^ lax.shift_right_logical(x, 15)
    x = x * 1863026059
    x = x ^ lax.shift_right_logical(x, 16)
    return (x & 65535).astype(jnp.float32)


def weigh_body(order_ref, ids_ref, w_ref, amp_ref, out_ref):
    for chan in range(w_ref.shape[1]):
        scale = amp_ref[chan : chan + 1, :] * (1.0 / 18918.0)
        out_ref[0, chan] = (w_ref[0, chan].astype(jnp.float32) * scale).astype(jnp.bfloat16)


def weigh(m_order, ids, singular_projection, noise_amp, part, chan):
    modes, pairs = singular_projection.shape[2:]
    count = m_order.shape[0] // 2
    return pl.pallas_call(
        weigh_body,
        out_shape=jax.ShapeDtypeStruct((count, chan, modes, pairs), jnp.bfloat16),
        grid_spec=pltpu.PrefetchScalarGridSpec(
            num_scalar_prefetch=2,
            grid=(count,),
            in_specs=[
                pl.BlockSpec((1, chan, modes, pairs), lambda i, m, ids: (m[2 * i + ids[1]], part, 0, 0)),
                pl.BlockSpec((chan, pairs), lambda i, m, ids: (part, 0)),
            ],
            out_specs=pl.BlockSpec((1, chan, modes, pairs), lambda i, m, ids: (i, 0, 0, 0)),
        ),
        compiler_params=pltpu.CompilerParams(dimension_semantics=("arbitrary",)),
        name="weigh",
    )(m_order, ids, singular_projection, noise_amp)


tile = 256


def draw_tiles(seed_ref, channel, pairs):
    base = (lax.broadcasted_iota(jnp.int32, (8, tile), 0) + channel * pairs) * golden
    for r0 in range(0, seed_ref.shape[1], tile):
        start = seed_ref[:, r0 : r0 + tile] + base
        for b0 in range(0, pairs, tile):
            bits = jnp.concatenate([draw_bits(start + wrap(b * golden)) for b in range(b0, b0 + tile, 8)], 0)
            yield r0, b0, bits.astype(jnp.bfloat16)


def channel_of(place, half, chan):
    return place // chan * (2 * chan) + half * chan + place % chan


def centre_of(w):
    return 32767.5 * jnp.sum(w.astype(jnp.float32), axis=1, keepdims=True)


def put_product(w, draws, r0, b0, pairs, total, centre, out_ref, place):
    piece = jnp.dot(w[:, b0 : b0 + tile], draws, preferred_element_type=jnp.float32)
    total = piece if b0 == 0 else total + piece
    if b0 + tile == pairs:
        out_ref[place, :, r0 : r0 + tile] = (total - centre).astype(jnp.bfloat16)
    return total


def draw_body(seed_ref, out_ref, *, first, half, chan, pairs):
    channel = channel_of(first + pl.program_id(0), half, chan)
    for r0, b0, draws in draw_tiles(seed_ref, channel, pairs):
        out_ref[0, b0 : b0 + tile, r0 : r0 + tile] = draws


def draw(seed_rows, first, count, half, chan, pairs):
    reals = seed_rows.shape[1]
    return pl.pallas_call(
        functools.partial(draw_body, first=first, half=half, chan=chan, pairs=pairs),
        out_shape=jax.ShapeDtypeStruct((count, pairs, reals), jnp.bfloat16),
        grid=(count,),
        in_specs=[pl.BlockSpec((8, reals), lambda i: (0, 0))],
        out_specs=pl.BlockSpec((1, pairs, reals), lambda i: (i, 0, 0)),
        compiler_params=pltpu.CompilerParams(dimension_semantics=("arbitrary",)),
        name="draw",
    )(seed_rows)


def project_body(seed_ref, w_ref, out_ref, *, first, half, chan):
    channel = channel_of(first + pl.program_id(0), half, chan)
    w = w_ref[0]
    pairs = w.shape[1]
    centre = centre_of(w)
    total = None
    for r0, b0, draws in draw_tiles(seed_ref, channel, pairs):
        total = put_product(w, draws, r0, b0, pairs, total, centre, out_ref, 0)


def project(seed_rows, weights, first, count, half, chan):
    modes, pairs = weights.shape[1:]
    reals = seed_rows.shape[1]
    return pl.pallas_call(
        functools.partial(project_body, first=first, half=half, chan=chan),
        out_shape=jax.ShapeDtypeStruct((count, modes, reals), jnp.bfloat16),
        grid=(count,),
        in_specs=[
            pl.BlockSpec((8, reals), lambda i: (0, 0)),
            pl.BlockSpec((1, modes, pairs), lambda i: (first + i, 0, 0)),
        ],
        out_specs=pl.BlockSpec((1, modes, reals), lambda i: (i, 0, 0)),
        compiler_params=pltpu.CompilerParams(dimension_semantics=("arbitrary",)),
        name="project",
    )(seed_rows, weights)


def finish_body(seed_ref, w_ref, held_ref, held_w_ref, out_ref, held_out_ref, *, first, half, chan, each):
    channel = channel_of(first + pl.program_id(0), half, chan)
    w = w_ref[0]
    pairs = w.shape[1]
    centre = centre_of(w)
    held_w = [held_w_ref[place] for place in range(each)]
    held_centre = [centre_of(one) for one in held_w]
    total = None
    held_total = [None] * each
    for r0, b0, draws in draw_tiles(seed_ref, channel, pairs):
        total = put_product(w, draws, r0, b0, pairs, total, centre, out_ref, 0)
        for place in range(each):
            kept = held_ref[place, b0 : b0 + tile, r0 : r0 + tile]
            held_total[place] = put_product(
                held_w[place], kept, r0, b0, pairs, held_total[place], held_centre[place], held_out_ref, place
            )


def finish(seed_rows, weights, held, first, count, half, chan, each):
    modes, pairs = weights.shape[1:]
    reals = seed_rows.shape[1]
    last = held.shape[0] // each - 1
    return pl.pallas_call(
        functools.partial(finish_body, first=first, half=half, chan=chan, each=each),
        out_shape=[
            jax.ShapeDtypeStruct((count, modes, reals), jnp.bfloat16),
            jax.ShapeDtypeStruct((held.shape[0], modes, reals), jnp.bfloat16),
        ],
        grid=(count,),
        in_specs=[
            pl.BlockSpec((8, reals), lambda i: (0, 0)),
            pl.BlockSpec((1, modes, pairs), lambda i: (first + i, 0, 0)),
            pl.BlockSpec((each, pairs, reals), lambda i: (jnp.minimum(i, last), 0, 0)),
            pl.BlockSpec((each, modes, pairs), lambda i: (jnp.minimum(i, last), 0, 0)),
        ],
        out_specs=[
            pl.BlockSpec((1, modes, reals), lambda i: (i, 0, 0)),
            pl.BlockSpec((each, modes, reals), lambda i: (jnp.minimum(i, last), 0, 0)),
        ],
        compiler_params=pltpu.CompilerParams(dimension_semantics=("arbitrary",), vmem_limit_bytes=32 * 2**20),
        name="finish",
    )(seed_rows, weights, held, weights)


def transform_body(ids_ref, order_ref, counts_ref, near_ref, far_ref, *refs, rows, blocks, modes):
    vec_refs, out_ref = refs[:-1], refs[-1]
    step = pl.program_id(0)
    first = step * rows
    limit = counts_ref[order_ref[2 * ids_ref[0] + ids_ref[1]]]
    mine = step // blocks == ids_ref[1]

    def run(kl_ref):
        total = None
        lead, *trail = vec_refs
        at = [(ref, k) for ref in trail for k in range(0, ref.shape[0], modes)]
        for k, (ref, start) in enumerate(at):
            piece = jnp.concatenate([lead[k * modes : (k + 1) * modes, :], ref[start : start + modes, :]], 0)
            part = jnp.dot(kl_ref[0, :, 2 * k * modes : 2 * (k + 1) * modes], piece, preferred_element_type=jnp.float32)
            total = part if total is None else total + part
        row = first + lax.broadcasted_iota(jnp.int32, total.shape, 0)
        out_ref[0] = jnp.where(row < limit, total, 0.0).astype(jnp.bfloat16)

    @pl.when((first < limit) & mine)
    def _():
        run(near_ref)

    @pl.when((first < limit) & jnp.logical_not(mine))
    def _():
        run(far_ref)

    @pl.when(first >= limit)
    def _():
        out_ref[...] = jnp.zeros(out_ref.shape, out_ref.dtype)


def transform(ids, m_order, mode_counts, kl_near, kl_far, vectors, modes, half, halves, slots):
    held, length = kl_near.shape[1:]
    reals = vectors[0].shape[1] // halves
    rows = 256
    blocks = held // rows

    def near(i, s, o, c):
        return (s[1], jnp.clip(i - s[1] * blocks, 0, blocks - 1), 0)

    def far(i, s, o, c):
        return (s[1], jnp.clip(i - (1 - s[1]) * blocks, 0, blocks - 1), 0)

    return pl.pallas_call(
        functools.partial(transform_body, rows=rows, blocks=blocks, modes=modes),
        out_shape=jax.ShapeDtypeStruct((slots, 2 * held, reals), jnp.bfloat16),
        grid_spec=pltpu.PrefetchScalarGridSpec(
            num_scalar_prefetch=3,
            grid=(2 * blocks,),
            in_specs=[
                pl.BlockSpec((1, rows, length), near),
                pl.BlockSpec((1, rows, length), far),
                *[pl.BlockSpec((v.shape[0], reals), lambda i, s, o, c: (0, half)) for v in vectors],
            ],
            out_specs=pl.BlockSpec((1, rows, reals), lambda i, s, o, c: (s[1] * (slots - 1), i, 0)),
        ),
        compiler_params=pltpu.CompilerParams(dimension_semantics=("arbitrary",), vmem_limit_bytes=48 * 2**20),
        name="transform",
    )(ids, m_order, mode_counts, kl_near, kl_far, *vectors)


def per_device(seeds, noise_amp, singular_projection, kl_vecs, m_order, mode_counts):
    d = lax.axis_index("freq")
    core = lax.axis_index("mgrp")
    modes, pairs = singular_projection.shape[2:]
    chan = singular_projection.shape[1] // 2
    ids = jnp.stack([d, core]).astype(jnp.int32)
    swap = [(0, 1), (1, 0)]

    pair = lax.dynamic_slice_in_dim(m_order, 2 * d, 2)
    own_seeds = lax.dynamic_index_in_dim(seeds, pair[core], 0)
    far_seeds = lax.ppermute(lax.dynamic_index_in_dim(seeds, pair[1 - core], 0), "mgrp", swap)
    seed_row = jnp.concatenate([own_seeds, far_seeds], 1)
    seed_rows = jnp.broadcast_to(seed_row, (8, seed_row.shape[1]))

    def exchange(order, half):
        sent = weigh(order, ids, singular_projection, noise_amp, half, chan)
        return lax.all_to_all(sent, "freq", split_axis=0, concat_axis=0, tiled=True).reshape(-1, modes, pairs)

    weights = exchange(m_order, 0)
    kl_far = lax.ppermute(kl_vecs, "mgrp", swap)
    total = weights.shape[0]
    ahead = total * 3 // 4
    held = draw(seed_rows, 0, ahead, 1, chan, pairs)
    late_order, held = lax.optimization_barrier((m_order, held))
    late_weights = exchange(late_order, 1)
    first = project(seed_rows, weights, 0, total, 0, chan)
    last, early = finish(seed_rows, late_weights, held, ahead, total - ahead, 1, chan, 3)

    vectors = [v.reshape(-1, v.shape[2]) for v in (first, early, last)]
    sent = transform(ids, m_order, mode_counts, kl_vecs, kl_far, vectors, chan * modes, 1, 2, 1)
    got = lax.ppermute(sent, "mgrp", swap)
    kept = transform(ids, m_order, mode_counts, kl_vecs, kl_far, vectors, chan * modes, 0, 2, 2)
    return lax.dynamic_update_slice_in_dim(kept, got, 1 - core, 0)


def solution(mesh):
    placed = (
        P("groups", "mgrp"),
        P(("groups", "freq"), None),
        P("groups", "freq", None, None),
        P(("groups", "freq"), "mgrp", None),
        P("groups"),
        P("groups"),
    )
    return jax.shard_map(
        per_device,
        mesh=mesh,
        in_specs=placed,
        out_specs=P(("groups", "freq"), None, "mgrp"),
        check_vma=False,
    )
```

```python
import functools

import jax
import jax.numpy as jnp
from jax import lax
from jax.experimental import pallas as pl
from jax.experimental.pallas import tpu as pltpu
from jax.sharding import PartitionSpec as P

golden = 1640531527
tile = 256


def wrap(value):
    value &= 0xFFFFFFFF
    return value - (1 << 32) if value >= 1 << 31 else value


def in_order(vmem=None):
    return pltpu.CompilerParams(
        dimension_semantics=("arbitrary",), vmem_limit_bytes=None if vmem is None else vmem * 2**20
    )


def draw_bits(x):
    x = x ^ lax.shift_right_logical(x, 16)
    x = x * 2146121005
    x = x ^ lax.shift_right_logical(x, 15)
    x = x * 1863026059
    x = x ^ lax.shift_right_logical(x, 16)
    return (x & 65535).astype(jnp.float32)


def pick_body(order_ref, ids_ref, seeds_ref, own_ref, sent_ref):
    first = 2 * ids_ref[0]
    own_ref[...] = jnp.broadcast_to(seeds_ref[pl.ds(order_ref[first + ids_ref[1]], 1), :], own_ref.shape)
    sent_ref[...] = jnp.broadcast_to(seeds_ref[pl.ds(order_ref[first + 1 - ids_ref[1]], 1), :], sent_ref.shape)


def pick(m_order, ids, seeds):
    rows = jax.ShapeDtypeStruct((8, seeds.shape[1]), seeds.dtype)
    smem = pl.BlockSpec(memory_space=pltpu.SMEM)
    vmem = pl.BlockSpec(memory_space=pltpu.VMEM)
    return pl.pallas_call(
        pick_body, out_shape=[rows, rows], in_specs=[smem, smem, vmem], out_specs=[vmem, vmem], name="pick"
    )(m_order, ids, seeds)


def weigh_body(order_ref, ids_ref, amp_ref, *refs):
    out_ref = refs[-1]
    for place, w_ref in enumerate(refs[:-1]):
        for chan in range(w_ref.shape[1]):
            scale = amp_ref[chan : chan + 1, :] * (1.0 / 18918.0)
            out_ref[place, chan] = (w_ref[0, chan].astype(jnp.float32) * scale).astype(jnp.bfloat16)


def weigh(m_order, ids, singular_projection, noise_amp, part, chan):
    modes, pairs = singular_projection.shape[2:]
    count = m_order.shape[0] // 2
    each = 4

    def rows_of(place):
        return pl.BlockSpec(
            (1, chan, modes, pairs), lambda i, m, ids: (m[2 * (each * i + place) + ids[1]], part, 0, 0)
        )

    return pl.pallas_call(
        weigh_body,
        out_shape=jax.ShapeDtypeStruct((count, chan, modes, pairs), jnp.bfloat16),
        grid_spec=pltpu.PrefetchScalarGridSpec(
            num_scalar_prefetch=2,
            grid=(count // each,),
            in_specs=[pl.BlockSpec((chan, pairs), lambda i, m, ids: (part, 0))] + [rows_of(k) for k in range(each)],
            out_specs=pl.BlockSpec((each, chan, modes, pairs), lambda i, m, ids: (i, 0, 0, 0)),
        ),
        compiler_params=in_order(),
        name="weigh",
    )(m_order, ids, noise_amp, *[singular_projection] * each)


def draw_tiles(seed_refs, channel, pairs):
    base = (lax.broadcasted_iota(jnp.int32, (8, tile), 0) + channel * pairs) * golden
    held = seed_refs[0].shape[1]
    for r0 in range(0, held * len(seed_refs), tile):
        start = seed_refs[r0 // held][:, r0 % held : r0 % held + tile] + base
        for b0 in range(0, pairs, tile):
            bits = jnp.concatenate([draw_bits(start + wrap(b * golden)) for b in range(b0, b0 + tile, 8)], 0)
            yield r0, b0, bits.astype(jnp.bfloat16)


def channel_of(place, half, chan):
    return place // chan * (2 * chan) + half * chan + place % chan


def centre_of(w):
    return 32767.5 * jnp.sum(w.astype(jnp.float32), axis=1, keepdims=True)


def put_product(w, draws, r0, b0, pairs, total, centre, out_ref, place):
    piece = jnp.dot(w[:, b0 : b0 + tile], draws, preferred_element_type=jnp.float32)
    total = piece if b0 == 0 else total + piece
    if b0 + tile == pairs:
        out_ref[place, :, r0 : r0 + tile] = (total - centre).astype(jnp.bfloat16)
    return total


def seed_spec(seeds):
    return pl.BlockSpec(seeds.shape, lambda i: (0, 0))


def draw_body(own_ref, far_ref, out_ref, *, first, half, chan):
    each, pairs = out_ref.shape[:2]
    for place in range(each):
        channel = channel_of(first + pl.program_id(0) * each + place, half, chan)
        for r0, b0, draws in draw_tiles((own_ref, far_ref), channel, pairs):
            out_ref[place, b0 : b0 + tile, r0 : r0 + tile] = draws


def draw(seeds, first, count, half, chan, pairs, each):
    reals = sum(s.shape[1] for s in seeds)
    return pl.pallas_call(
        functools.partial(draw_body, first=first, half=half, chan=chan),
        out_shape=jax.ShapeDtypeStruct((count, pairs, reals), jnp.bfloat16),
        grid=(count // each,),
        in_specs=[seed_spec(s) for s in seeds],
        out_specs=pl.BlockSpec((each, pairs, reals), lambda i: (i, 0, 0)),
        compiler_params=in_order(32),
        name="draw",
    )(*seeds)


def project_body(own_ref, far_ref, w_ref, out_ref, *, first, half, chan):
    each, _, pairs = w_ref.shape
    for place in range(each):
        channel = channel_of(first + pl.program_id(0) * each + place, half, chan)
        w = w_ref[place]
        centre = centre_of(w)
        total = None
        for r0, b0, draws in draw_tiles((own_ref, far_ref), channel, pairs):
            total = put_product(w, draws, r0, b0, pairs, total, centre, out_ref, place)


def project(seeds, weights, first, count, half, chan, each):
    modes, pairs = weights.shape[1:]
    reals = sum(s.shape[1] for s in seeds)
    return pl.pallas_call(
        functools.partial(project_body, first=first, half=half, chan=chan),
        out_shape=jax.ShapeDtypeStruct((count, modes, reals), jnp.bfloat16),
        grid=(count // each,),
        in_specs=[seed_spec(s) for s in seeds]
        + [pl.BlockSpec((each, modes, pairs), lambda i: (first // each + i, 0, 0))],
        out_specs=pl.BlockSpec((each, modes, reals), lambda i: (i, 0, 0)),
        compiler_params=in_order(),
        name="project",
    )(*seeds, weights)


def finish_body(own_ref, far_ref, w_ref, held_ref, held_w_ref, out_ref, held_out_ref, *, first, half, chan):
    each, _, pairs = w_ref.shape
    held_each = held_ref.shape[0] // each
    for place in range(each):
        channel = channel_of(first + pl.program_id(0) * each + place, half, chan)
        w = w_ref[place]
        centre = centre_of(w)
        kept = range(place * held_each, (place + 1) * held_each)
        held_w = [held_w_ref[k] for k in kept]
        held_centre = [centre_of(one) for one in held_w]
        total = None
        held_total = [None] * held_each
        for r0, b0, draws in draw_tiles((own_ref, far_ref), channel, pairs):
            total = put_product(w, draws, r0, b0, pairs, total, centre, out_ref, place)
            for n, k in enumerate(kept):
                old = held_ref[k, b0 : b0 + tile, r0 : r0 + tile]
                held_total[n] = put_product(
                    held_w[n], old, r0, b0, pairs, held_total[n], held_centre[n], held_out_ref, k
                )


def finish(seeds, weights, held, half, chan, each):
    modes, pairs = weights.shape[1:]
    reals = sum(s.shape[1] for s in seeds)
    first = held.shape[0]
    count = weights.shape[0] - first
    steps = count // each
    held_each = first // steps
    return pl.pallas_call(
        functools.partial(finish_body, first=first, half=half, chan=chan),
        out_shape=[
            jax.ShapeDtypeStruct((count, modes, reals), jnp.bfloat16),
            jax.ShapeDtypeStruct((first, modes, reals), jnp.bfloat16),
        ],
        grid=(steps,),
        in_specs=[seed_spec(s) for s in seeds]
        + [
            pl.BlockSpec((each, modes, pairs), lambda i: (first // each + i, 0, 0)),
            pl.BlockSpec((held_each, pairs, reals), lambda i: (i, 0, 0)),
            pl.BlockSpec((held_each, modes, pairs), lambda i: (i, 0, 0)),
        ],
        out_specs=[
            pl.BlockSpec((each, modes, reals), lambda i: (i, 0, 0)),
            pl.BlockSpec((held_each, modes, reals), lambda i: (i, 0, 0)),
        ],
        compiler_params=in_order(48),
        name="finish",
    )(*seeds, weights, held, weights)


def transform_body(ids_ref, order_ref, counts_ref, near_ref, far_ref, lead_ref, early_ref, last_ref, out_ref, sum_ref, *, cut):
    step = pl.program_id(0)
    held = near_ref.shape[1]

    @pl.when(step == 0)
    def _():
        sum_ref[...] = jnp.zeros(sum_ref.shape, sum_ref.dtype)

    trail = jnp.where(step < cut, early_ref[...], last_ref[...])
    vectors = jnp.concatenate([lead_ref[...], trail], 0)
    for place, kl_ref in enumerate((near_ref, far_ref)):
        sum_ref[place] += jnp.dot(kl_ref[0], vectors, preferred_element_type=jnp.float32)

    @pl.when(step == pl.num_programs(0) - 1)
    def _():
        limit = counts_ref[order_ref[2 * ids_ref[0] + ids_ref[1]]]
        for place in range(2):
            first = (ids_ref[1] if place == 0 else 1 - ids_ref[1]) * held
            first = pl.multiple_of(first, held)
            row = first + lax.broadcasted_iota(jnp.int32, sum_ref.shape[1:], 0)
            coeffs = jnp.where(row < limit, sum_ref[place], 0.0).astype(jnp.bfloat16)
            out_ref[0, pl.ds(first, held), :] = coeffs


def transform(ids, m_order, mode_counts, kl_near, kl_far, vectors, rows, half, halves, slots):
    held, length = kl_near.shape[1:]
    reals = vectors[0].shape[1] // halves
    cut = vectors[1].shape[0] // rows

    def kl_rows(i, s, o, c):
        return (s[1], 0, i)

    return pl.pallas_call(
        functools.partial(transform_body, cut=cut),
        out_shape=jax.ShapeDtypeStruct((slots, 2 * held, reals), jnp.bfloat16),
        grid_spec=pltpu.PrefetchScalarGridSpec(
            num_scalar_prefetch=3,
            grid=(length // (2 * rows),),
            in_specs=[
                pl.BlockSpec((1, held, 2 * rows), kl_rows),
                pl.BlockSpec((1, held, 2 * rows), kl_rows),
                pl.BlockSpec((rows, reals), lambda i, s, o, c: (i, half)),
                pl.BlockSpec((rows, reals), lambda i, s, o, c: (jnp.minimum(i, cut - 1), half)),
                pl.BlockSpec((rows, reals), lambda i, s, o, c: (jnp.maximum(i - cut, 0), half)),
            ],
            out_specs=pl.BlockSpec((1, 2 * held, reals), lambda i, s, o, c: (s[1] * (slots - 1), 0, 0)),
            scratch_shapes=[pltpu.VMEM((2, held, reals), jnp.float32)],
        ),
        compiler_params=in_order(32),
        name="transform",
    )(ids, m_order, mode_counts, kl_near, kl_far, *vectors)


def per_device(seeds, noise_amp, singular_projection, kl_vecs, m_order, mode_counts):
    d = lax.axis_index("freq")
    core = lax.axis_index("mgrp")
    modes, pairs = singular_projection.shape[2:]
    chan = singular_projection.shape[1] // 2
    ids = jnp.stack([d, core]).astype(jnp.int32)
    swap = [(0, 1), (1, 0)]

    own_seeds, sent_seeds = pick(m_order, ids, seeds)
    far_seeds = lax.ppermute(sent_seeds, "mgrp", swap)

    def exchange(sent):
        return lax.all_to_all(sent, "freq", split_axis=0, concat_axis=0, tiled=True).reshape(-1, modes, pairs)

    sent = weigh(m_order, ids, singular_projection, noise_amp, 0, chan)
    sent, far_seeds, kl_sent = lax.optimization_barrier((sent, far_seeds, kl_vecs))
    both_seeds = (own_seeds, far_seeds)
    weights = exchange(sent)
    kl_far = lax.ppermute(kl_sent, "mgrp", swap)
    total = weights.shape[0]
    ahead = total * 3 // 4
    held = draw(both_seeds, 0, ahead, 1, chan, pairs, 4)
    late_order, held = lax.optimization_barrier((m_order, held))
    late_weights = exchange(weigh(late_order, ids, singular_projection, noise_amp, 1, chan))
    first = project(both_seeds, weights, 0, total, 0, chan, 4)
    last, early = finish(both_seeds, late_weights, held, 1, chan, 2)

    vectors = [v.reshape(-1, v.shape[2]) for v in (first, early, last)]
    rows = chan * modes
    sent = transform(ids, m_order, mode_counts, kl_vecs, kl_far, vectors, rows, 1, 2, 1)
    got = lax.ppermute(sent, "mgrp", swap)
    kept = transform(ids, m_order, mode_counts, kl_vecs, kl_far, vectors, rows, 0, 2, 2)
    return lax.dynamic_update_slice_in_dim(kept, got, 1 - core, 0)


def solution(mesh):
    placed = (
        P("groups", "mgrp"),
        P(("groups", "freq"), None),
        P("groups", "freq", None, None),
        P(("groups", "freq"), "mgrp", None),
        P("groups"),
        P("groups"),
    )
    return jax.shard_map(
        per_device,
        mesh=mesh,
        in_specs=placed,
        out_specs=P(("groups", "freq"), None, "mgrp"),
        check_vma=False,
    )
```

```python
import functools

import jax
import jax.numpy as jnp
from jax import lax
from jax.experimental import pallas as pl
from jax.experimental.pallas import tpu as pltpu
from jax.sharding import PartitionSpec as P


golden = 1640531527
tile = 256


def wrap(value):
    value &= 0xFFFFFFFF
    return value - (1 << 32) if value >= 1 << 31 else value


def in_order(vmem=None):
    return pltpu.CompilerParams(
        dimension_semantics=("arbitrary",), vmem_limit_bytes=None if vmem is None else vmem * 2**20
    )


def draw_bits(x):
    x = x ^ lax.shift_right_logical(x, 16)
    x = x * 2146121005
    x = x ^ lax.shift_right_logical(x, 15)
    x = x * 1863026059
    x = x ^ lax.shift_right_logical(x, 16)
    return (x & 65535).astype(jnp.float32)


def pick_body(order_ref, ids_ref, seeds_ref, own_ref, sent_ref):
    first = 2 * ids_ref[0]
    own_ref[...] = jnp.broadcast_to(seeds_ref[pl.ds(order_ref[first + ids_ref[1]], 1), :], own_ref.shape)
    sent_ref[...] = jnp.broadcast_to(seeds_ref[pl.ds(order_ref[first + 1 - ids_ref[1]], 1), :], sent_ref.shape)


def pick(m_order, ids, seeds):
    rows = jax.ShapeDtypeStruct((8, seeds.shape[1]), seeds.dtype)
    smem = pl.BlockSpec(memory_space=pltpu.SMEM)
    vmem = pl.BlockSpec(memory_space=pltpu.VMEM)
    return pl.pallas_call(
        pick_body, out_shape=[rows, rows], in_specs=[smem, smem, vmem], out_specs=[vmem, vmem], name="pick"
    )(m_order, ids, seeds)


def weigh_body(order_ref, ids_ref, amp_ref, *refs):
    out_ref = refs[-1]
    for place, w_ref in enumerate(refs[:-1]):
        for chan in range(w_ref.shape[1]):
            scale = amp_ref[chan : chan + 1, :] * (1.0 / 18918.0)
            out_ref[place, chan] = (w_ref[0, chan].astype(jnp.float32) * scale).astype(jnp.bfloat16)


def weigh(m_order, ids, singular_projection, noise_amp, part, chan):
    modes, pairs = singular_projection.shape[2:]
    count = m_order.shape[0] // 2
    each = 4

    def rows_of(place):
        return pl.BlockSpec(
            (1, chan, modes, pairs), lambda i, m, ids: (m[2 * (each * i + place) + ids[1]], part, 0, 0)
        )

    return pl.pallas_call(
        weigh_body,
        out_shape=jax.ShapeDtypeStruct((count, chan, modes, pairs), jnp.bfloat16),
        grid_spec=pltpu.PrefetchScalarGridSpec(
            num_scalar_prefetch=2,
            grid=(count // each,),
            in_specs=[pl.BlockSpec((chan, pairs), lambda i, m, ids: (part, 0))] + [rows_of(k) for k in range(each)],
            out_specs=pl.BlockSpec((each, chan, modes, pairs), lambda i, m, ids: (i, 0, 0, 0)),
        ),
        compiler_params=in_order(),
        name="weigh",
    )(m_order, ids, noise_amp, *[singular_projection] * each)


def draw_tiles(seed_refs, channel, pairs):
    base = (lax.broadcasted_iota(jnp.int32, (8, tile), 0) + channel * pairs) * golden
    held = seed_refs[0].shape[1]
    for r0 in range(0, held * len(seed_refs), tile):
        start = seed_refs[r0 // held][:, r0 % held : r0 % held + tile] + base
        for b0 in range(0, pairs, tile):
            bits = jnp.concatenate([draw_bits(start + wrap(b * golden)) for b in range(b0, b0 + tile, 8)], 0)
            yield r0, b0, bits.astype(jnp.bfloat16)


def channel_of(place, half, chan):
    return place // chan * (2 * chan) + half * chan + place % chan


def centre_of(w):
    return 32767.5 * jnp.sum(w.astype(jnp.float32), axis=1, keepdims=True)


def put_product(w, draws, r0, b0, pairs, total, centre, out_ref, place):
    piece = jnp.dot(w[:, b0 : b0 + tile], draws, preferred_element_type=jnp.float32)
    total = piece if b0 == 0 else total + piece
    if b0 + tile == pairs:
        out_ref[place, :, r0 : r0 + tile] = (total - centre).astype(jnp.bfloat16)
    return total


def seed_spec(seeds):
    return pl.BlockSpec(seeds.shape, lambda i: (0, 0))


def draw_body(own_ref, far_ref, out_ref, *, first, half, chan):
    each, pairs = out_ref.shape[:2]
    for place in range(each):
        channel = channel_of(first + pl.program_id(0) * each + place, half, chan)
        for r0, b0, draws in draw_tiles((own_ref, far_ref), channel, pairs):
            out_ref[place, b0 : b0 + tile, r0 : r0 + tile] = draws


def draw(seeds, first, count, half, chan, pairs, each):
    reals = sum(s.shape[1] for s in seeds)
    return pl.pallas_call(
        functools.partial(draw_body, first=first, half=half, chan=chan),
        out_shape=jax.ShapeDtypeStruct((count, pairs, reals), jnp.bfloat16),
        grid=(count // each,),
        in_specs=[seed_spec(s) for s in seeds],
        out_specs=pl.BlockSpec((each, pairs, reals), lambda i: (i, 0, 0)),
        compiler_params=in_order(60),
        name="draw",
    )(*seeds)


def project_body(ids_ref, own_ref, far_ref, w_ref, *refs, half, chan, local):
    out_ref = refs[-1]
    each, _, pairs = w_ref.shape
    block = block_of(pl.program_id(0), ids_ref, chan // each, local)
    for place in range(each):
        channel = channel_of(block * each + place, half, chan)
        w = w_ref[place]
        centre = centre_of(w)
        total = None
        for r0, b0, draws in draw_tiles((own_ref, far_ref), channel, pairs):
            total = put_product(w, draws, r0, b0, pairs, total, centre, out_ref, place)


def block_of(step, ids, blocks, local):
    if local:
        return ids[0] * blocks + step
    chip = step // blocks
    return (chip + (chip >= ids[0]).astype(jnp.int32)) * blocks + step % blocks


def project(ids, seeds, weights, vectors, half, chan, each, local):
    count, modes, pairs = weights.shape
    reals = sum(s.shape[1] for s in seeds)
    blocks = chan // each
    steps = blocks if local else count // each - blocks

    def at(i, ids):
        return (block_of(i, ids, blocks, local), 0, 0)

    operands = [ids, *seeds, weights]
    in_specs = [pl.BlockSpec(s.shape, lambda i, ids: (0, 0)) for s in seeds]
    in_specs += [pl.BlockSpec((each, modes, pairs), at)]
    aliases = {}
    if vectors is not None:
        aliases = {len(operands): 0}
        operands.append(vectors)
        in_specs.append(pl.BlockSpec(memory_space=pl.ANY))
    return pl.pallas_call(
        functools.partial(project_body, half=half, chan=chan, local=local),
        out_shape=jax.ShapeDtypeStruct((count, modes, reals), jnp.bfloat16),
        grid_spec=pltpu.PrefetchScalarGridSpec(
            num_scalar_prefetch=1,
            grid=(steps,),
            in_specs=in_specs,
            out_specs=pl.BlockSpec((each, modes, reals), at),
        ),
        input_output_aliases=aliases,
        compiler_params=in_order(60),
        name="near" if local else "project",
    )(*operands)


def finish_body(own_ref, far_ref, w_ref, held_ref, held_w_ref, out_ref, held_out_ref, *, first, half, chan):
    each, _, pairs = w_ref.shape
    held_each = held_ref.shape[0] // each
    for place in range(each):
        channel = channel_of(first + pl.program_id(0) * each + place, half, chan)
        w = w_ref[place]
        centre = centre_of(w)
        kept = range(place * held_each, (place + 1) * held_each)
        held_w = [held_w_ref[k] for k in kept]
        held_centre = [centre_of(one) for one in held_w]
        total = None
        held_total = [None] * held_each
        for r0, b0, draws in draw_tiles((own_ref, far_ref), channel, pairs):
            total = put_product(w, draws, r0, b0, pairs, total, centre, out_ref, place)
            for n, k in enumerate(kept):
                old = held_ref[k, b0 : b0 + tile, r0 : r0 + tile]
                held_total[n] = put_product(
                    held_w[n], old, r0, b0, pairs, held_total[n], held_centre[n], held_out_ref, k
                )


def finish(seeds, weights, held, half, chan, each):
    modes, pairs = weights.shape[1:]
    reals = sum(s.shape[1] for s in seeds)
    first = held.shape[0]
    count = weights.shape[0] - first
    steps = count // each
    held_each = first // steps
    return pl.pallas_call(
        functools.partial(finish_body, first=first, half=half, chan=chan),
        out_shape=[
            jax.ShapeDtypeStruct((count, modes, reals), jnp.bfloat16),
            jax.ShapeDtypeStruct((first, modes, reals), jnp.bfloat16),
        ],
        grid=(steps,),
        in_specs=[seed_spec(s) for s in seeds]
        + [
            pl.BlockSpec((each, modes, pairs), lambda i: (first // each + i, 0, 0)),
            pl.BlockSpec((held_each, pairs, reals), lambda i: (i, 0, 0)),
            pl.BlockSpec((held_each, modes, pairs), lambda i: (i, 0, 0)),
        ],
        out_specs=[
            pl.BlockSpec((each, modes, reals), lambda i: (i, 0, 0)),
            pl.BlockSpec((held_each, modes, reals), lambda i: (i, 0, 0)),
        ],
        compiler_params=in_order(60),
        name="finish",
    )(*seeds, weights, held, weights)


def transform_body(ids_ref, order_ref, counts_ref, near_ref, far_ref, *refs, rows, blocks, modes):
    vec_refs, out_ref = refs[:-1], refs[-1]
    step = pl.program_id(0)
    first = step * rows
    limit = counts_ref[order_ref[2 * ids_ref[0] + ids_ref[1]]]
    mine = step // blocks == ids_ref[1]

    def run(kl_ref):
        total = None
        lead, *trail = vec_refs
        at = [(ref, k) for ref in trail for k in range(0, ref.shape[0], modes)]
        for k, (ref, start) in enumerate(at):
            piece = jnp.concatenate([lead[k * modes : (k + 1) * modes, :], ref[start : start + modes, :]], 0)
            part = jnp.dot(kl_ref[0, :, 2 * k * modes : 2 * (k + 1) * modes], piece, preferred_element_type=jnp.float32)
            total = part if total is None else total + part
        row = first + lax.broadcasted_iota(jnp.int32, total.shape, 0)
        out_ref[0] = jnp.where(row < limit, total, 0.0).astype(jnp.bfloat16)

    @pl.when((first < limit) & mine)
    def _():
        run(near_ref)

    @pl.when((first < limit) & jnp.logical_not(mine))
    def _():
        run(far_ref)

    @pl.when(first >= limit)
    def _():
        out_ref[...] = jnp.zeros(out_ref.shape, out_ref.dtype)


def transform(ids, m_order, mode_counts, kl_near, kl_far, vectors, modes, half, halves, slots):
    held, length = kl_near.shape[1:]
    reals = vectors[0].shape[1] // halves
    rows = 256
    blocks = held // rows

    def near(i, s, o, c):
        return (s[1], jnp.clip(i - s[1] * blocks, 0, blocks - 1), 0)

    def far(i, s, o, c):
        return (s[1], jnp.clip(i - (1 - s[1]) * blocks, 0, blocks - 1), 0)

    return pl.pallas_call(
        functools.partial(transform_body, rows=rows, blocks=blocks, modes=modes),
        out_shape=jax.ShapeDtypeStruct((slots, 2 * held, reals), jnp.bfloat16),
        grid_spec=pltpu.PrefetchScalarGridSpec(
            num_scalar_prefetch=3,
            grid=(2 * blocks,),
            in_specs=[
                pl.BlockSpec((1, rows, length), near),
                pl.BlockSpec((1, rows, length), far),
                *[pl.BlockSpec((v.shape[0], reals), lambda i, s, o, c: (0, half)) for v in vectors],
            ],
            out_specs=pl.BlockSpec((1, rows, reals), lambda i, s, o, c: (s[1] * (slots - 1), i, 0)),
        ),
        compiler_params=in_order(60),
        name="transform",
    )(ids, m_order, mode_counts, kl_near, kl_far, *vectors)


def per_device(seeds, noise_amp, singular_projection, kl_vecs, m_order, mode_counts):
    d = lax.axis_index("freq")
    core = lax.axis_index("mgrp")
    modes, pairs = singular_projection.shape[2:]
    chan = singular_projection.shape[1] // 2
    ids = jnp.stack([d, core]).astype(jnp.int32)
    swap = [(0, 1), (1, 0)]

    own_seeds, sent_seeds = pick(m_order, ids, seeds)
    far_seeds = lax.ppermute(sent_seeds, "mgrp", swap)

    def exchange(sent):
        return lax.all_to_all(sent, "freq", split_axis=0, concat_axis=0, tiled=True).reshape(-1, modes, pairs)

    sent = weigh(m_order, ids, singular_projection, noise_amp, 0, chan)
    sent, far_seeds, kl_sent = lax.optimization_barrier((sent, far_seeds, kl_vecs))
    both_seeds = (own_seeds, far_seeds)
    weights = exchange(sent)
    kl_far = lax.ppermute(kl_sent, "mgrp", swap)
    ahead = weights.shape[0] * 3 // 4
    held = draw(both_seeds, 0, ahead, 1, chan, pairs, 4)
    near = project(ids, both_seeds, sent.reshape(-1, modes, pairs), None, 0, chan, 4, True)
    late_order, held, near = lax.optimization_barrier((m_order, held, near))
    late_weights = exchange(weigh(late_order, ids, singular_projection, noise_amp, 1, chan))
    first = project(ids, both_seeds, weights, near, 0, chan, 8, False)
    last, early = finish(both_seeds, late_weights, held, 1, chan, 2)

    vectors = [v.reshape(-1, v.shape[2]) for v in (first, early, last)]
    rows = chan * modes
    sent = transform(ids, m_order, mode_counts, kl_vecs, kl_far, vectors, rows, 1, 2, 1)
    got = lax.ppermute(sent, "mgrp", swap)
    kept = transform(ids, m_order, mode_counts, kl_vecs, kl_far, vectors, rows, 0, 2, 2)
    return lax.dynamic_update_slice_in_dim(kept, got, 1 - core, 0)


def solution(mesh):
    placed = (
        P("groups", "mgrp"),
        P(("groups", "freq"), None),
        P("groups", "freq", None, None),
        P(("groups", "freq"), "mgrp", None),
        P("groups"),
        P("groups"),
    )
    return jax.shard_map(
        per_device,
        mesh=mesh,
        in_specs=placed,
        out_specs=P(("groups", "freq"), None, "mgrp"),
        check_vma=False,
    )
```

```python
import functools

import jax
import jax.numpy as jnp
from jax import lax
from jax.experimental import pallas as pl
from jax.experimental.pallas import tpu as pltpu
from jax.sharding import PartitionSpec as P


golden = 1640531527
tile = 256
FULL = 63


def wrap(value):
    value &= 0xFFFFFFFF
    return value - (1 << 32) if value >= 1 << 31 else value


def in_order(vmem=None):
    return pltpu.CompilerParams(
        dimension_semantics=("arbitrary",), vmem_limit_bytes=None if vmem is None else vmem * 2**20
    )


def draw_bits(x):
    x = x ^ lax.shift_right_logical(x, 16)
    x = x * 2146121005
    x = x ^ lax.shift_right_logical(x, 15)
    x = x * 1863026059
    x = x ^ lax.shift_right_logical(x, 16)
    return (x & 65535).astype(jnp.float32)


def pick_body(order_ref, ids_ref, seeds_ref, own_ref, sent_ref):
    first = 2 * ids_ref[0]
    own_ref[...] = jnp.broadcast_to(seeds_ref[pl.ds(order_ref[first + ids_ref[1]], 1), :], own_ref.shape)
    sent_ref[...] = jnp.broadcast_to(seeds_ref[pl.ds(order_ref[first + 1 - ids_ref[1]], 1), :], sent_ref.shape)


def pick(m_order, ids, seeds):
    rows = jax.ShapeDtypeStruct((8, seeds.shape[1]), seeds.dtype)
    smem = pl.BlockSpec(memory_space=pltpu.SMEM)
    vmem = pl.BlockSpec(memory_space=pltpu.VMEM)
    return pl.pallas_call(
        pick_body, out_shape=[rows, rows], in_specs=[smem, smem, vmem], out_specs=[vmem, vmem], name="pick"
    )(m_order, ids, seeds)


def weigh_body(order_ref, ids_ref, amp_ref, *refs):
    out_ref = refs[-1]
    for place, w_ref in enumerate(refs[:-1]):
        for chan in range(w_ref.shape[1]):
            scale = amp_ref[chan : chan + 1, :] * (1.0 / 18918.0)
            out_ref[place, chan] = (w_ref[0, chan].astype(jnp.float32) * scale).astype(jnp.bfloat16)


def weigh(m_order, ids, singular_projection, noise_amp, part, chan):
    modes, pairs = singular_projection.shape[2:]
    count = m_order.shape[0] // 2
    each = 8

    def rows_of(place):
        return pl.BlockSpec(
            (1, chan, modes, pairs), lambda i, m, ids: (m[2 * (each * i + place) + ids[1]], part, 0, 0)
        )

    return pl.pallas_call(
        weigh_body,
        out_shape=jax.ShapeDtypeStruct((count, chan, modes, pairs), jnp.bfloat16),
        grid_spec=pltpu.PrefetchScalarGridSpec(
            num_scalar_prefetch=2,
            grid=(count // each,),
            in_specs=[pl.BlockSpec((chan, pairs), lambda i, m, ids: (part, 0))] + [rows_of(k) for k in range(each)],
            out_specs=pl.BlockSpec((each, chan, modes, pairs), lambda i, m, ids: (i, 0, 0, 0)),
        ),
        compiler_params=in_order(FULL),
        name="weigh",
    )(m_order, ids, noise_amp, *[singular_projection] * each)


def draw_tiles(seed_refs, channel, pairs):
    base = (lax.broadcasted_iota(jnp.int32, (8, tile), 0) + channel * pairs) * golden
    held = seed_refs[0].shape[1]
    for r0 in range(0, held * len(seed_refs), tile):
        start = seed_refs[r0 // held][:, r0 % held : r0 % held + tile] + base
        for b0 in range(0, pairs, tile):
            bits = jnp.concatenate([draw_bits(start + wrap(b * golden)) for b in range(b0, b0 + tile, 8)], 0)
            yield r0, b0, bits.astype(jnp.bfloat16)


def channel_of(place, half, chan):
    return place // chan * (2 * chan) + half * chan + place % chan


def centre_of(w):
    return 32767.5 * jnp.sum(w.astype(jnp.float32), axis=1, keepdims=True)


def put_product(w, draws, r0, b0, pairs, total, centre, out_ref, place):
    piece = jnp.dot(w[:, b0 : b0 + tile], draws, preferred_element_type=jnp.float32)
    total = piece if b0 == 0 else total + piece
    if b0 + tile == pairs:
        out_ref[place, :, r0 : r0 + tile] = (total - centre).astype(jnp.bfloat16)
    return total


def seed_spec(seeds):
    return pl.BlockSpec(seeds.shape, lambda i: (0, 0))


def draw_body(own_ref, far_ref, out_ref, *, first, half, chan):
    each, pairs = out_ref.shape[:2]
    for place in range(each):
        channel = channel_of(first + pl.program_id(0) * each + place, half, chan)
        for r0, b0, draws in draw_tiles((own_ref, far_ref), channel, pairs):
            out_ref[place, b0 : b0 + tile, r0 : r0 + tile] = draws


def draw(seeds, first, count, half, chan, pairs, each):
    reals = sum(s.shape[1] for s in seeds)
    return pl.pallas_call(
        functools.partial(draw_body, first=first, half=half, chan=chan),
        out_shape=jax.ShapeDtypeStruct((count, pairs, reals), jnp.bfloat16),
        grid=(count // each,),
        in_specs=[seed_spec(s) for s in seeds],
        out_specs=pl.BlockSpec((each, pairs, reals), lambda i: (i, 0, 0)),
        compiler_params=in_order(FULL),
        name="draw",
    )(*seeds)


def project_body(ids_ref, own_ref, far_ref, w_ref, *refs, half, chan, local):
    out_ref = refs[-1]
    each, _, pairs = w_ref.shape
    block = block_of(pl.program_id(0), ids_ref, chan // each, local)
    for place in range(each):
        channel = channel_of(block * each + place, half, chan)
        w = w_ref[place]
        centre = centre_of(w)
        total = None
        for r0, b0, draws in draw_tiles((own_ref, far_ref), channel, pairs):
            total = put_product(w, draws, r0, b0, pairs, total, centre, out_ref, place)


def block_of(step, ids, blocks, local):
    if local:
        return ids[0] * blocks + step
    chip = step // blocks
    return (chip + (chip >= ids[0]).astype(jnp.int32)) * blocks + step % blocks


def project(ids, seeds, weights, vectors, half, chan, each, local):
    count, modes, pairs = weights.shape
    reals = sum(s.shape[1] for s in seeds)
    blocks = chan // each
    steps = blocks if local else count // each - blocks

    def at(i, ids):
        return (block_of(i, ids, blocks, local), 0, 0)

    operands = [ids, *seeds, weights]
    in_specs = [pl.BlockSpec(s.shape, lambda i, ids: (0, 0)) for s in seeds]
    in_specs += [pl.BlockSpec((each, modes, pairs), at)]
    aliases = {}
    if vectors is not None:
        aliases = {len(operands): 0}
        operands.append(vectors)
        in_specs.append(pl.BlockSpec(memory_space=pl.ANY))
    return pl.pallas_call(
        functools.partial(project_body, half=half, chan=chan, local=local),
        out_shape=jax.ShapeDtypeStruct((count, modes, reals), jnp.bfloat16),
        grid_spec=pltpu.PrefetchScalarGridSpec(
            num_scalar_prefetch=1,
            grid=(steps,),
            in_specs=in_specs,
            out_specs=pl.BlockSpec((each, modes, reals), at),
        ),
        input_output_aliases=aliases,
        compiler_params=in_order(FULL),
        name="near" if local else "project",
    )(*operands)


def turn(step, steps, fetch):
    @pl.when(step == 0)
    def _():
        for ahead in range(2):
            fetch(ahead, ahead, True)

    @pl.when(step + 2 < steps)
    def _():
        fetch(step + 2, lax.rem(step + 2, 3), True)

    slot = lax.rem(step, 3)
    fetch(step, slot, False)
    return slot


def finish_body(own_ref, far_ref, w_ref, held_hbm, held_w_ref, out_ref, held_out_ref, ring_ref, sems, *, first, half, chan):
    each, _, pairs = w_ref.shape
    step_held = ring_ref.shape[1]
    held_each = step_held // each

    def fetch(step, slot, start):
        copy = pltpu.make_async_copy(held_hbm.at[pl.ds(step * step_held, step_held)], ring_ref.at[slot], sems.at[slot])
        copy.start() if start else copy.wait()

    slot = turn(pl.program_id(0), held_hbm.shape[0] // step_held, fetch)
    for place in range(each):
        channel = channel_of(first + pl.program_id(0) * each + place, half, chan)
        w = w_ref[place]
        centre = centre_of(w)
        kept = range(place * held_each, (place + 1) * held_each)
        held_w = [held_w_ref[k] for k in kept]
        held_centre = [centre_of(one) for one in held_w]
        total = None
        held_total = [None] * held_each
        for r0, b0, draws in draw_tiles((own_ref, far_ref), channel, pairs):
            total = put_product(w, draws, r0, b0, pairs, total, centre, out_ref, place)
            for n, k in enumerate(kept):
                old = ring_ref[slot, k, b0 : b0 + tile, r0 : r0 + tile]
                held_total[n] = put_product(
                    held_w[n], old, r0, b0, pairs, held_total[n], held_centre[n], held_out_ref, k
                )


def finish(seeds, weights, held, half, chan, each):
    modes, pairs = weights.shape[1:]
    reals = sum(s.shape[1] for s in seeds)
    first = held.shape[0]
    count = weights.shape[0] - first
    steps = count // each
    held_each = first // steps
    return pl.pallas_call(
        functools.partial(finish_body, first=first, half=half, chan=chan),
        out_shape=[
            jax.ShapeDtypeStruct((count, modes, reals), jnp.bfloat16),
            jax.ShapeDtypeStruct((first, modes, reals), jnp.bfloat16),
        ],
        grid=(steps,),
        in_specs=[seed_spec(s) for s in seeds]
        + [
            pl.BlockSpec((each, modes, pairs), lambda i: (first // each + i, 0, 0)),
            pl.BlockSpec(memory_space=pl.ANY),
            pl.BlockSpec((held_each, modes, pairs), lambda i: (i, 0, 0)),
        ],
        out_specs=[
            pl.BlockSpec((each, modes, reals), lambda i: (i, 0, 0)),
            pl.BlockSpec((held_each, modes, reals), lambda i: (i, 0, 0)),
        ],
        scratch_shapes=[pltpu.VMEM((3, held_each, pairs, reals), held.dtype), pltpu.SemaphoreType.DMA((3,))],
        compiler_params=in_order(FULL),
        name="finish",
    )(*seeds, weights, held, weights)


def transform_body(ids_ref, order_ref, counts_ref, near_hbm, far_hbm, *refs, modes):
    *vec_refs, out_ref, ring_ref, sems = refs
    step = pl.program_id(0)
    rows = ring_ref.shape[1]
    blocks = near_hbm.shape[1] // rows
    core = ids_ref[1]
    limit = counts_ref[order_ref[2 * ids_ref[0] + core]]

    def fetch(step, slot, start):
        block = step if isinstance(step, int) else lax.rem(step, blocks)

        def copy_from(ref):
            return pltpu.make_async_copy(ref.at[core, pl.ds(block * rows, rows)], ring_ref.at[slot], sems.at[slot])

        if not start:
            copy_from(near_hbm).wait()
            return
        mine = core == step // blocks

        @pl.when(mine)
        def _():
            copy_from(near_hbm).start()

        @pl.when(jnp.logical_not(mine))
        def _():
            copy_from(far_hbm).start()

    slot = turn(step, 2 * blocks, fetch)
    first = step * rows

    @pl.when(first < limit)
    def _():
        total = None
        lead, *trail = vec_refs
        at = [(ref, k) for ref in trail for k in range(0, ref.shape[0], modes)]
        for k, (ref, start) in enumerate(at):
            piece = jnp.concatenate([lead[k * modes : (k + 1) * modes, :], ref[start : start + modes, :]], 0)
            columns = ring_ref[slot, :, 2 * k * modes : 2 * (k + 1) * modes]
            part = jnp.dot(columns, piece, preferred_element_type=jnp.float32)
            total = part if total is None else total + part
        row = first + lax.broadcasted_iota(jnp.int32, total.shape, 0)
        out_ref[0] = jnp.where(row < limit, total, 0.0).astype(jnp.bfloat16)

    @pl.when(first >= limit)
    def _():
        out_ref[...] = jnp.zeros(out_ref.shape, out_ref.dtype)


def transform(ids, m_order, mode_counts, kl_near, kl_far, vectors, modes, half, halves, slots):
    held, length = kl_near.shape[1:]
    reals = vectors[0].shape[1] // halves
    rows = 256
    return pl.pallas_call(
        functools.partial(transform_body, modes=modes),
        out_shape=jax.ShapeDtypeStruct((slots, 2 * held, reals), jnp.bfloat16),
        grid_spec=pltpu.PrefetchScalarGridSpec(
            num_scalar_prefetch=3,
            grid=(2 * held // rows,),
            in_specs=[
                pl.BlockSpec(memory_space=pl.ANY),
                pl.BlockSpec(memory_space=pl.ANY),
                *[pl.BlockSpec((v.shape[0], reals), lambda i, s, o, c: (0, half)) for v in vectors],
            ],
            out_specs=pl.BlockSpec((1, rows, reals), lambda i, s, o, c: (s[1] * (slots - 1), i, 0)),
            scratch_shapes=[pltpu.VMEM((3, rows, length), kl_near.dtype), pltpu.SemaphoreType.DMA((3,))],
        ),
        compiler_params=in_order(FULL),
        name="transform",
    )(ids, m_order, mode_counts, kl_near, kl_far, *vectors)


def per_device(seeds, noise_amp, singular_projection, kl_vecs, m_order, mode_counts):
    d = lax.axis_index("freq")
    core = lax.axis_index("mgrp")
    modes, pairs = singular_projection.shape[2:]
    chan = singular_projection.shape[1] // 2
    ids = jnp.stack([d, core]).astype(jnp.int32)
    swap = [(0, 1), (1, 0)]

    own_seeds, sent_seeds = pick(m_order, ids, seeds)
    far_seeds = lax.ppermute(sent_seeds, "mgrp", swap)

    def exchange(sent):
        return lax.all_to_all(sent, "freq", split_axis=0, concat_axis=0, tiled=True).reshape(-1, modes, pairs)

    sent = weigh(m_order, ids, singular_projection, noise_amp, 0, chan)
    sent, far_seeds, kl_sent = lax.optimization_barrier((sent, far_seeds, kl_vecs))
    both_seeds = (own_seeds, far_seeds)
    weights = exchange(sent)
    kl_far = lax.ppermute(kl_sent, "mgrp", swap)
    ahead = weights.shape[0] * 3 // 4
    held = draw(both_seeds, 0, ahead, 1, chan, pairs, 4)
    near = project(ids, both_seeds, sent.reshape(-1, modes, pairs), None, 0, chan, 4, True)
    late_order, held, near = lax.optimization_barrier((m_order, held, near))
    late_weights = exchange(weigh(late_order, ids, singular_projection, noise_amp, 1, chan))
    first = project(ids, both_seeds, weights, near, 0, chan, 8, False)
    last, early = finish(both_seeds, late_weights, held, 1, chan, 2)

    vectors = [v.reshape(-1, v.shape[2]) for v in (first, early, last)]
    rows = chan * modes
    sent = transform(ids, m_order, mode_counts, kl_vecs, kl_far, vectors, rows, 1, 2, 1)
    got = lax.ppermute(sent, "mgrp", swap)
    kept = transform(ids, m_order, mode_counts, kl_vecs, kl_far, vectors, rows, 0, 2, 2)
    return lax.dynamic_update_slice_in_dim(kept, got, 1 - core, 0)


def solution(mesh):
    placed = (
        P("groups", "mgrp"),
        P(("groups", "freq"), None),
        P("groups", "freq", None, None),
        P(("groups", "freq"), "mgrp", None),
        P("groups"),
        P("groups"),
    )
    return jax.shard_map(
        per_device,
        mesh=mesh,
        in_specs=placed,
        out_specs=P(("groups", "freq"), None, "mgrp"),
        check_vma=False,
    )
```

```python
import functools

import jax
import jax.numpy as jnp
from jax import lax
from jax.experimental import pallas as pl
from jax.experimental.pallas import tpu as pltpu
from jax.sharding import PartitionSpec as P


golden = 1640531527
tile = 256
FULL = 63


def wrap(value):
    value &= 0xFFFFFFFF
    return value - (1 << 32) if value >= 1 << 31 else value


def in_order(vmem=None):
    return pltpu.CompilerParams(
        dimension_semantics=("arbitrary",), vmem_limit_bytes=None if vmem is None else vmem * 2**20
    )


def draw_bits(x):
    x = x ^ lax.shift_right_logical(x, 16)
    x = x * 2146121005
    x = x ^ lax.shift_right_logical(x, 15)
    x = x * 1863026059
    x = x ^ lax.shift_right_logical(x, 16)
    return (x & 65535).astype(jnp.float32)


def pick_body(order_ref, ids_ref, seeds_ref, own_ref, sent_ref):
    first = 2 * ids_ref[0]
    own_ref[...] = jnp.broadcast_to(seeds_ref[pl.ds(order_ref[first + ids_ref[1]], 1), :], own_ref.shape)
    sent_ref[...] = jnp.broadcast_to(seeds_ref[pl.ds(order_ref[first + 1 - ids_ref[1]], 1), :], sent_ref.shape)


def pick(m_order, ids, seeds):
    rows = jax.ShapeDtypeStruct((8, seeds.shape[1]), seeds.dtype)
    smem = pl.BlockSpec(memory_space=pltpu.SMEM)
    vmem = pl.BlockSpec(memory_space=pltpu.VMEM)
    return pl.pallas_call(
        pick_body, out_shape=[rows, rows], in_specs=[smem, smem, vmem], out_specs=[vmem, vmem], name="pick"
    )(m_order, ids, seeds)


def weigh_body(order_ref, ids_ref, amp_ref, *refs):
    out_ref = refs[-1]
    for place, w_ref in enumerate(refs[:-1]):
        for chan in range(w_ref.shape[1]):
            scale = amp_ref[chan : chan + 1, :] * (1.0 / 18918.0)
            out_ref[place, chan] = (w_ref[0, chan].astype(jnp.float32) * scale).astype(jnp.bfloat16)


def weigh(m_order, ids, singular_projection, noise_amp, part, chan):
    modes, pairs = singular_projection.shape[2:]
    count = m_order.shape[0] // 2
    each = 8

    def rows_of(place):
        return pl.BlockSpec(
            (1, chan, modes, pairs), lambda i, m, ids: (m[2 * (each * i + place) + ids[1]], part, 0, 0)
        )

    return pl.pallas_call(
        weigh_body,
        out_shape=jax.ShapeDtypeStruct((count, chan, modes, pairs), jnp.bfloat16),
        grid_spec=pltpu.PrefetchScalarGridSpec(
            num_scalar_prefetch=2,
            grid=(count // each,),
            in_specs=[pl.BlockSpec((chan, pairs), lambda i, m, ids: (part, 0))] + [rows_of(k) for k in range(each)],
            out_specs=pl.BlockSpec((each, chan, modes, pairs), lambda i, m, ids: (i, 0, 0, 0)),
        ),
        compiler_params=in_order(FULL),
        name="weigh",
    )(m_order, ids, noise_amp, *[singular_projection] * each)


def draw_tiles(seed_refs, channel, pairs):
    base = (lax.broadcasted_iota(jnp.int32, (8, tile), 0) + channel * pairs) * golden
    held = seed_refs[0].shape[1]
    for r0 in range(0, held * len(seed_refs), tile):
        start = seed_refs[r0 // held][:, r0 % held : r0 % held + tile] + base
        for b0 in range(0, pairs, tile):
            bits = jnp.concatenate([draw_bits(start + wrap(b * golden)) for b in range(b0, b0 + tile, 8)], 0)
            yield r0, b0, bits.astype(jnp.bfloat16)


def channel_of(place, half, chan):
    return place // chan * (2 * chan) + half * chan + place % chan


def centre_of(w):
    return 32767.5 * jnp.sum(w.astype(jnp.float32), axis=1, keepdims=True)


def put_product(w, draws, r0, b0, pairs, total, centre, out_ref, place):
    piece = jnp.dot(w[:, b0 : b0 + tile], draws, preferred_element_type=jnp.float32)
    total = piece if b0 == 0 else total + piece
    if b0 + tile == pairs:
        out_ref[place, :, r0 : r0 + tile] = (total - centre).astype(jnp.bfloat16)
    return total


def seed_spec(seeds):
    return pl.BlockSpec(seeds.shape, lambda i: (0, 0))


def draw_body(own_ref, far_ref, out_ref, *, first, half, chan):
    each, pairs = out_ref.shape[:2]
    for place in range(each):
        channel = channel_of(first + pl.program_id(0) * each + place, half, chan)
        for r0, b0, draws in draw_tiles((own_ref, far_ref), channel, pairs):
            out_ref[place, b0 : b0 + tile, r0 : r0 + tile] = draws


def draw(seeds, first, count, half, chan, pairs, each):
    reals = sum(s.shape[1] for s in seeds)
    return pl.pallas_call(
        functools.partial(draw_body, first=first, half=half, chan=chan),
        out_shape=jax.ShapeDtypeStruct((count, pairs, reals), jnp.bfloat16),
        grid=(count // each,),
        in_specs=[seed_spec(s) for s in seeds],
        out_specs=pl.BlockSpec((each, pairs, reals), lambda i: (i, 0, 0)),
        compiler_params=in_order(FULL),
        name="draw",
    )(*seeds)


def project_body(ids_ref, own_ref, far_ref, w_ref, *refs, half, chan, local):
    out_ref = refs[-1]
    each, _, pairs = w_ref.shape
    block = block_of(pl.program_id(0), ids_ref, chan // each, local)
    for place in range(each):
        channel = channel_of(block * each + place, half, chan)
        w = w_ref[place]
        centre = centre_of(w)
        total = None
        for r0, b0, draws in draw_tiles((own_ref, far_ref), channel, pairs):
            total = put_product(w, draws, r0, b0, pairs, total, centre, out_ref, place)


def block_of(step, ids, blocks, local):
    if local:
        return ids[0] * blocks + step
    chip = step // blocks
    return (chip + (chip >= ids[0]).astype(jnp.int32)) * blocks + step % blocks


def project(ids, seeds, weights, vectors, half, chan, each, local):
    count, modes, pairs = weights.shape
    reals = sum(s.shape[1] for s in seeds)
    blocks = chan // each
    steps = blocks if local else count // each - blocks

    def at(i, ids):
        return (block_of(i, ids, blocks, local), 0, 0)

    operands = [ids, *seeds, weights]
    in_specs = [pl.BlockSpec(s.shape, lambda i, ids: (0, 0)) for s in seeds]
    in_specs += [pl.BlockSpec((each, modes, pairs), at)]
    aliases = {}
    if vectors is not None:
        aliases = {len(operands): 0}
        operands.append(vectors)
        in_specs.append(pl.BlockSpec(memory_space=pl.ANY))
    return pl.pallas_call(
        functools.partial(project_body, half=half, chan=chan, local=local),
        out_shape=jax.ShapeDtypeStruct((count, modes, reals), jnp.bfloat16),
        grid_spec=pltpu.PrefetchScalarGridSpec(
            num_scalar_prefetch=1,
            grid=(steps,),
            in_specs=in_specs,
            out_specs=pl.BlockSpec((each, modes, reals), at),
        ),
        input_output_aliases=aliases,
        compiler_params=in_order(FULL),
        name="near" if local else "project",
    )(*operands)


def turn(step, steps, fetch):
    @pl.when(step == 0)
    def _():
        for ahead in range(2):
            fetch(ahead, ahead, True)

    @pl.when(step + 2 < steps)
    def _():
        fetch(step + 2, lax.rem(step + 2, 3), True)

    slot = lax.rem(step, 3)
    fetch(step, slot, False)
    return slot


def finish_body(own_ref, far_ref, w_ref, held_hbm, held_w_ref, out_ref, held_out_ref, ring_ref, sems, *, first, half, chan):
    each, _, pairs = w_ref.shape
    step_held = ring_ref.shape[1]
    held_each = step_held // each

    def fetch(step, slot, start):
        copy = pltpu.make_async_copy(held_hbm.at[pl.ds(step * step_held, step_held)], ring_ref.at[slot], sems.at[slot])
        copy.start() if start else copy.wait()

    slot = turn(pl.program_id(0), held_hbm.shape[0] // step_held, fetch)
    for place in range(each):
        channel = channel_of(first + pl.program_id(0) * each + place, half, chan)
        w = w_ref[place]
        centre = centre_of(w)
        kept = range(place * held_each, (place + 1) * held_each)
        held_w = [held_w_ref[k] for k in kept]
        held_centre = [centre_of(one) for one in held_w]
        total = None
        held_total = [None] * held_each
        for r0, b0, draws in draw_tiles((own_ref, far_ref), channel, pairs):
            total = put_product(w, draws, r0, b0, pairs, total, centre, out_ref, place)
            for n, k in enumerate(kept):
                old = ring_ref[slot, k, b0 : b0 + tile, r0 : r0 + tile]
                held_total[n] = put_product(
                    held_w[n], old, r0, b0, pairs, held_total[n], held_centre[n], held_out_ref, k
                )


def finish(seeds, weights, held, half, chan, each):
    modes, pairs = weights.shape[1:]
    reals = sum(s.shape[1] for s in seeds)
    first = held.shape[0]
    count = weights.shape[0] - first
    steps = count // each
    held_each = first // steps
    return pl.pallas_call(
        functools.partial(finish_body, first=first, half=half, chan=chan),
        out_shape=[
            jax.ShapeDtypeStruct((count, modes, reals), jnp.bfloat16),
            jax.ShapeDtypeStruct((first, modes, reals), jnp.bfloat16),
        ],
        grid=(steps,),
        in_specs=[seed_spec(s) for s in seeds]
        + [
            pl.BlockSpec((each, modes, pairs), lambda i: (first // each + i, 0, 0)),
            pl.BlockSpec(memory_space=pl.ANY),
            pl.BlockSpec((held_each, modes, pairs), lambda i: (i, 0, 0)),
        ],
        out_specs=[
            pl.BlockSpec((each, modes, reals), lambda i: (i, 0, 0)),
            pl.BlockSpec((held_each, modes, reals), lambda i: (i, 0, 0)),
        ],
        scratch_shapes=[pltpu.VMEM((3, held_each, pairs, reals), held.dtype), pltpu.SemaphoreType.DMA((3,))],
        compiler_params=in_order(FULL),
        name="finish",
    )(*seeds, weights, held, weights)


def transform_body(ids_ref, order_ref, counts_ref, near_hbm, far_hbm, *refs, modes, half):
    count = (len(refs) - 4) // 2
    vec_hbm, out_ref, vec_refs = refs[:count], refs[count], refs[count + 1 : 2 * count + 1]
    ring_ref, sems, vec_sems = refs[2 * count + 1 :]
    step = pl.program_id(0)
    rows = ring_ref.shape[1]
    blocks = near_hbm.shape[1] // rows
    core = ids_ref[1]
    limit = counts_ref[order_ref[2 * ids_ref[0] + core]]

    def fetch(step, slot, start):
        block = step if isinstance(step, int) else lax.rem(step, blocks)

        def copy_from(ref):
            return pltpu.make_async_copy(ref.at[core, pl.ds(block * rows, rows)], ring_ref.at[slot], sems.at[slot])

        if not start:
            copy_from(near_hbm).wait()
            return
        mine = core == step // blocks

        @pl.when(mine)
        def _():
            copy_from(near_hbm).start()

        @pl.when(jnp.logical_not(mine))
        def _():
            copy_from(far_hbm).start()

    def vectors():
        for n, (src, dst) in enumerate(zip(vec_hbm, vec_refs)):
            reals = dst.shape[1]
            yield pltpu.make_async_copy(src.at[:, pl.ds(half * reals, reals)], dst, vec_sems.at[n])

    @pl.when(step == 0)
    def _():
        for copy in vectors():
            copy.start()

    slot = turn(step, 2 * blocks, fetch)

    @pl.when(step == 0)
    def _():
        for copy in vectors():
            copy.wait()

    first = step * rows

    @pl.when(first < limit)
    def _():
        total = None
        lead, *trail = vec_refs
        at = [(ref, k) for ref in trail for k in range(0, ref.shape[0], modes)]
        for k, (ref, start) in enumerate(at):
            piece = jnp.concatenate([lead[k * modes : (k + 1) * modes, :], ref[start : start + modes, :]], 0)
            columns = ring_ref[slot, :, 2 * k * modes : 2 * (k + 1) * modes]
            part = jnp.dot(columns, piece, preferred_element_type=jnp.float32)
            total = part if total is None else total + part
        row = first + lax.broadcasted_iota(jnp.int32, total.shape, 0)
        out_ref[0] = jnp.where(row < limit, total, 0.0).astype(jnp.bfloat16)

    @pl.when(first >= limit)
    def _():
        out_ref[...] = jnp.zeros(out_ref.shape, out_ref.dtype)


def transform(ids, m_order, mode_counts, kl_near, kl_far, vectors, modes, half, halves, slots):
    held, length = kl_near.shape[1:]
    reals = vectors[0].shape[1] // halves
    rows = 256
    return pl.pallas_call(
        functools.partial(transform_body, modes=modes, half=half),
        out_shape=jax.ShapeDtypeStruct((slots, 2 * held, reals), jnp.bfloat16),
        grid_spec=pltpu.PrefetchScalarGridSpec(
            num_scalar_prefetch=3,
            grid=(2 * held // rows,),
            in_specs=[
                pl.BlockSpec(memory_space=pl.ANY),
                pl.BlockSpec(memory_space=pl.ANY),
                *[pl.BlockSpec(memory_space=pl.ANY) for v in vectors],
            ],
            out_specs=pl.BlockSpec((1, rows, reals), lambda i, s, o, c: (s[1] * (slots - 1), i, 0)),
            scratch_shapes=[
                *[pltpu.VMEM((v.shape[0], reals), v.dtype) for v in vectors],
                pltpu.VMEM((3, rows, length), kl_near.dtype),
                pltpu.SemaphoreType.DMA((3,)),
                pltpu.SemaphoreType.DMA((len(vectors),)),
            ],
        ),
        compiler_params=in_order(60),
        name="transform",
    )(ids, m_order, mode_counts, kl_near, kl_far, *vectors)


def per_device(seeds, noise_amp, singular_projection, kl_vecs, m_order, mode_counts):
    d = lax.axis_index("freq")
    core = lax.axis_index("mgrp")
    modes, pairs = singular_projection.shape[2:]
    chan = singular_projection.shape[1] // 2
    ids = jnp.stack([d, core]).astype(jnp.int32)
    swap = [(0, 1), (1, 0)]

    own_seeds, sent_seeds = pick(m_order, ids, seeds)
    far_seeds = lax.ppermute(sent_seeds, "mgrp", swap)

    def exchange(sent):
        return lax.all_to_all(sent, "freq", split_axis=0, concat_axis=0, tiled=True).reshape(-1, modes, pairs)

    sent = weigh(m_order, ids, singular_projection, noise_amp, 0, chan)
    sent, far_seeds, kl_sent = lax.optimization_barrier((sent, far_seeds, kl_vecs))
    both_seeds = (own_seeds, far_seeds)
    weights = exchange(sent)
    kl_far = lax.ppermute(kl_sent, "mgrp", swap)
    ahead = weights.shape[0] * 3 // 4
    held = draw(both_seeds, 0, ahead, 1, chan, pairs, 4)
    near = project(ids, both_seeds, sent.reshape(-1, modes, pairs), None, 0, chan, 4, True)
    late_order, held, near = lax.optimization_barrier((m_order, held, near))
    late_weights = exchange(weigh(late_order, ids, singular_projection, noise_amp, 1, chan))
    first = project(ids, both_seeds, weights, near, 0, chan, 8, False)
    last, early = finish(both_seeds, late_weights, held, 1, chan, 2)

    vectors = [v.reshape(-1, v.shape[2]) for v in (first, early, last)]
    rows = chan * modes
    sent = transform(ids, m_order, mode_counts, kl_vecs, kl_far, vectors, rows, 1, 2, 1)
    got = lax.ppermute(sent, "mgrp", swap)
    kept = transform(ids, m_order, mode_counts, kl_vecs, kl_far, vectors, rows, 0, 2, 2)
    return lax.dynamic_update_slice_in_dim(kept, got, 1 - core, 0)


def solution(mesh):
    placed = (
        P("groups", "mgrp"),
        P(("groups", "freq"), None),
        P("groups", "freq", None, None),
        P(("groups", "freq"), "mgrp", None),
        P("groups"),
        P("groups"),
    )
    return jax.shard_map(
        per_device,
        mesh=mesh,
        in_specs=placed,
        out_specs=P(("groups", "freq"), None, "mgrp"),
        check_vma=False,
    )
```
